256 devices in a mesh: graph: 256 (over z, y, x, core).
Axes of the slice: x: 4, y: 4, z: 8, core: 2. Of those that a mesh axis runs over, the one named last changes fastest.
Arguments:
- feats: bfloat16 [1048576, 200], P('graph')
- w_one: float32 [200, 512], replicated
- w_two: float32 [512, 107], replicated
- send_idx: int32 [65536, 4], P('graph')
- send_count: int32 [65536], P('graph')
- edge_src: int32 [1048576, 8], P('graph')
- edge_wt: float32 [1048576, 8], P('graph')
- labels: int32 [1048576], P('graph')
- label_mask: int32 [1048576], P('graph')
Outputs:
- output 1: float32 [], replicated
- output 2: float32 [200, 512], replicated
- output 3: float32 [512, 107], replicated
All inputs are finite; a program needn't handle non-finite values.
Results may differ from the reference program's by a relative error of at most 0.001.
Values are sent between devices in bfloat16 or wider.
A program may use at most 768 MiB of HBM per device.

```python
import jax
import jax.numpy as jnp
from jax import lax

GRAPH_DEVS = 256
ROWS_DEV = 4096
HALO_ROWS = 4
IN_DEG = 8
FEAT_IN = 200
FEAT_HID = 512
CLASSES = 107

TOTAL_ROWS = GRAPH_DEVS * ROWS_DEV
EXT_ROWS = ROWS_DEV + GRAPH_DEVS * HALO_ROWS


def draw_structure(rng_key):
    rng_keys = jax.random.split(rng_key, 7)
    dev_ids = jnp.arange(GRAPH_DEVS)
    skew_a = jax.random.randint(rng_keys[0], (GRAPH_DEVS, GRAPH_DEVS), 0, HALO_ROWS)
    skew_b = jax.random.randint(rng_keys[1], (GRAPH_DEVS, GRAPH_DEVS), 0, HALO_ROWS)
    counts = 1 + (skew_a * skew_b) // HALO_ROWS
    full_list = dev_ids[None, :] == (dev_ids[:, None] + 1) % GRAPH_DEVS
    counts = jnp.where(full_list, HALO_ROWS, counts)
    send_idx = jax.random.randint(rng_keys[2], (GRAPH_DEVS * GRAPH_DEVS, HALO_ROWS), 0, ROWS_DEV)
    edge_shape = (GRAPH_DEVS, ROWS_DEV, IN_DEG)
    is_cut = jax.random.randint(rng_keys[3], edge_shape, 0, 4) == 0
    local_src = jax.random.randint(rng_keys[4], edge_shape, 0, ROWS_DEV)
    peer_dev = (dev_ids[:, None, None] + jax.random.randint(rng_keys[5], edge_shape, 1, GRAPH_DEVS)) % GRAPH_DEVS
    peer_count = counts[peer_dev, dev_ids[:, None, None]]
    slot_pos = jax.random.randint(rng_keys[6], edge_shape, 0, 1048576) % peer_count
    halo_src = ROWS_DEV + peer_dev * HALO_ROWS + slot_pos
    edge_src = jnp.where(is_cut, halo_src, local_src).reshape(TOTAL_ROWS, IN_DEG)
    return send_idx, counts.reshape(GRAPH_DEVS * GRAPH_DEVS), edge_src, is_cut.reshape(TOTAL_ROWS, IN_DEG)


def setup_inputs(seed: int = 0) -> dict:
    rng_keys = jax.random.split(jax.random.key(seed), 7)
    feats = jax.random.normal(rng_keys[0], (TOTAL_ROWS, FEAT_IN), jnp.float32).astype(jnp.bfloat16)
    w_one = jax.random.normal(rng_keys[1], (FEAT_IN, FEAT_HID), jnp.float32) * FEAT_IN ** -0.5
    w_two = jax.random.normal(rng_keys[2], (FEAT_HID, CLASSES), jnp.float32) * FEAT_HID ** -0.5
    send_idx, send_count, edge_src, is_cut = draw_structure(rng_keys[3])
    raw_wt = jax.random.uniform(rng_keys[4], (TOTAL_ROWS, IN_DEG), jnp.float32, 0.5, 1.5) * jnp.where(is_cut, 0.5, 1.0)
    edge_wt = raw_wt / jnp.sqrt(jnp.sum(raw_wt * raw_wt, axis=1, keepdims=True))
    labels = jax.random.randint(rng_keys[5], (TOTAL_ROWS,), 0, CLASSES)
    label_mask = jax.random.randint(rng_keys[6], (TOTAL_ROWS,), 0, 2)
    return {"feats": feats, "w_one": w_one, "w_two": w_two, "send_idx": send_idx, "send_count": send_count, "edge_src": edge_src, "edge_wt": edge_wt, "labels": labels, "label_mask": label_mask}


def reference(feats, w_one, w_two, send_idx, send_count, edge_src, edge_wt, labels, label_mask):
    dev_ids = jnp.arange(GRAPH_DEVS)
    send_lists = send_idx.reshape(GRAPH_DEVS, GRAPH_DEVS, HALO_ROWS) + (dev_ids * ROWS_DEV)[:, None, None]
    is_valid = (jnp.arange(HALO_ROWS)[None, None, :] < send_count.reshape(GRAPH_DEVS, GRAPH_DEVS)[:, :, None]).astype(jnp.float32)
    halo_ids = jnp.transpose(send_lists, (1, 0, 2)).reshape(GRAPH_DEVS, GRAPH_DEVS * HALO_ROWS)
    halo_ok = jnp.transpose(is_valid, (1, 0, 2)).reshape(GRAPH_DEVS, GRAPH_DEVS * HALO_ROWS)
    src_dev = edge_src.reshape(GRAPH_DEVS, ROWS_DEV, IN_DEG)
    wt_dev = edge_wt.reshape(GRAPH_DEVS, ROWS_DEV, IN_DEG)

    def aggregate(h_flat):
        feat_width = h_flat.shape[1]

        def one_dev(per_dev):
            own_rows, src_ids, edge_w, ids_here, ok_here = per_dev
            halo_vals = h_flat[ids_here].astype(jnp.float32) * ok_here[:, None]
            ext_rows = jnp.concatenate([own_rows.astype(jnp.float32), halo_vals], axis=0)
            return jnp.sum(ext_rows[src_ids] * edge_w[:, :, None], axis=1)

        blocks = h_flat.reshape(GRAPH_DEVS, ROWS_DEV, feat_width)
        return lax.map(one_dev, (blocks, src_dev, wt_dev, halo_ids, halo_ok)).reshape(TOTAL_ROWS, feat_width)

    def scatter_back(d_z):
        feat_width = d_z.shape[1]

        def one_dev(per_dev):
            src_ids, edge_w, dz_rows = per_dev
            contrib = (edge_w[:, :, None] * dz_rows[:, None, :]).reshape(ROWS_DEV * IN_DEG, feat_width)
            return jax.ops.segment_sum(contrib, src_ids.reshape(ROWS_DEV * IN_DEG), num_segments=EXT_ROWS)

        ext_grad = lax.map(one_dev, (src_dev, wt_dev, d_z.reshape(GRAPH_DEVS, ROWS_DEV, feat_width)))
        own_grad = ext_grad[:, :ROWS_DEV].reshape(TOTAL_ROWS, feat_width)
        halo_grad = ext_grad[:, ROWS_DEV:] * halo_ok[:, :, None]
        back_sum = jax.ops.segment_sum(halo_grad.reshape(GRAPH_DEVS * GRAPH_DEVS * HALO_ROWS, feat_width), halo_ids.reshape(GRAPH_DEVS * GRAPH_DEVS * HALO_ROWS), num_segments=TOTAL_ROWS)
        return own_grad + back_sum

    w_one_b = w_one.astype(jnp.bfloat16)
    w_two_b = w_two.astype(jnp.bfloat16)
    z_one = aggregate(feats).astype(jnp.bfloat16)
    h_one = jnp.maximum(jnp.dot(z_one, w_one_b, preferred_element_type=jnp.float32), 0.0).astype(jnp.bfloat16)
    z_two = aggregate(h_one).astype(jnp.bfloat16)
    logits = jnp.dot(z_two, w_two_b, preferred_element_type=jnp.float32)
    mask_f = label_mask.astype(jnp.float32)
    label_total = jnp.sum(mask_f)
    log_prob = jax.nn.log_softmax(logits, axis=-1)
    onehot = (labels[:, None] == jnp.arange(CLASSES)[None, :]).astype(jnp.float32)
    loss_val = -jnp.sum(mask_f[:, None] * onehot * log_prob) / label_total
    d_logits = ((jnp.exp(log_prob) - onehot) * (mask_f / label_total)[:, None]).astype(jnp.bfloat16)
    grad_two = jnp.dot(z_two.T, d_logits, preferred_element_type=jnp.float32)
    d_z2 = jnp.dot(d_logits, w_two_b.T, preferred_element_type=jnp.float32)
    d_h1 = scatter_back(d_z2)
    d_y1 = jnp.where(h_one > 0, d_h1, 0.0).astype(jnp.bfloat16)
    grad_one = jnp.dot(z_one.T, d_y1, preferred_element_type=jnp.float32)
    return (loss_val, grad_one, grad_two)
```

```python
import functools

import jax
import jax.numpy as jnp
from jax import lax
from jax.experimental import pallas as pl
from jax.experimental.pallas import tpu as pltpu
from jax.sharding import PartitionSpec as P


F32, BF16, I32 = jnp.float32, jnp.bfloat16, jnp.int32
LANES = 128
CHUNK_ROWS = 128
HIDDEN_ROWS = 256
CHUNKS = 4
VMEM_CAP = 60 * 2**20
MESH = pl.DeviceIdType.MESH


def params(**kw):
    return pltpu.CompilerParams(vmem_limit_bytes=VMEM_CAP, **kw)


def spread_rows(dst, rows_ref, base, width):
    parts = width // LANES
    count = rows_ref.shape[0]

    block = 128

    def body(i, _):
        r = pl.multiple_of(i * block, block)
        vals = rows_ref[pl.ds(r, block), :].astype(F32)
        for c in range(parts):
            dst[pl.ds((base + r) * parts + c, block, stride=parts), :] = vals[:, c * LANES:(c + 1) * LANES]
        return 0

    lax.fori_loop(0, count // block, body, 0)


def spread_lists(dst, lists_ref, base, parts):
    count, size = lists_ref.shape[:2]
    group = 16

    def body(i, _):
        for u in range(group):
            q = i * group + u
            vals = lists_ref[q].astype(F32)
            for c in range(parts):
                dst[pl.ds((base + q * size) * parts + c, size, stride=parts), :] = vals[:, c * LANES:(c + 1) * LANES]
        return 0

    lax.fori_loop(0, count // group, body, 0)


def join_parts(src, rows, parts):
    return jnp.concatenate([src[pl.ds(c, rows, stride=parts), :].astype(BF16) for c in range(parts)], axis=1)


def pick_kernel(idx, rows_ref, out, ext, stage):
    count = rows_ref.shape[0]
    lists, size = out.shape[:2]
    picks = lists * size
    gap = picks + 8
    group = 128 // size
    ext[pl.ds(2 * count, 8), :] = jnp.zeros((8, LANES), F32)
    spread_rows(ext, rows_ref, 0, 2 * LANES)

    def body(i, _):
        lo = idx.at[pl.ds(pl.multiple_of(i * 128, 128), 128)]
        for u in range(128):
            stage[pl.ds(i * 128 + u, 2, stride=gap), :] = ext[pl.ds(pl.multiple_of(lo[u], 2), 2), :]
        for u in range(group):
            for c in range(2):
                vals = stage[pl.ds(c * gap + i * 128 + u * size, size), :]
                out[i * group + u, :, c * LANES:(c + 1) * LANES] = vals.astype(BF16)
        return 0

    lax.fori_loop(0, picks // 128, body, 0)


def pick_rows(idx, rows, size):
    picks, count = idx.shape[0], rows.shape[0]
    return pl.pallas_call(
        pick_kernel,
        in_specs=[pl.BlockSpec(memory_space=pltpu.SMEM), pl.BlockSpec(memory_space=pltpu.VMEM)],
        out_specs=pl.BlockSpec(memory_space=pltpu.VMEM),
        out_shape=jax.ShapeDtypeStruct((picks // size, size, 2 * LANES), BF16),
        scratch_shapes=[pltpu.VMEM((2 * count + 8, LANES), F32), pltpu.VMEM((2 * (picks + 8), LANES), F32)],
        compiler_params=params(),
        name="pick_rows",
    )(idx, rows)


def index_copies(step, src, bufs, sems):
    size = bufs[0].shape[0]
    return [
        pltpu.make_async_copy(src.at[pl.ds(pl.multiple_of((step * CHUNKS + b) * size, size), size)], bufs[b], sems.at[b])
        for b in range(CHUNKS)
    ]


def with_indices(src, bufs, sems, visit):
    step, last = pl.program_id(0), pl.num_programs(0) - 1
    now, later = index_copies(step, src, bufs, sems), index_copies(step + 1, src, bufs, sems)

    @pl.when(step == 0)
    def _():
        for copy in now:
            copy.start()

    for b in range(CHUNKS):
        now[b].wait()
        visit(b, bufs[b])

        @pl.when(step < last)
        def _():
            later[b].start()


def weighted_rows(ext, wts, acc, parts, deg, b, idx):
    for n in range(CHUNK_ROWS):
        total = None
        for k in range(deg):
            row = ext[pl.ds(pl.multiple_of(idx[n * deg + k], parts), parts), :]
            term = row * wts[pl.ds((b * CHUNK_ROWS + n) * deg + k, 1), :]
            total = term if total is None else total + term
        acc[pl.ds((b * CHUNK_ROWS + n) * parts, parts), :] = total


def layer_one_kernel(deg, src, wts, own, halo, z_out, ext, acc, sems, *bufs):
    @pl.when(pl.program_id(0) == 0)
    def _():
        spread_rows(ext, own, 0, 2 * LANES)
        spread_lists(ext, halo, own.shape[0], 2)

    with_indices(src, bufs, sems, functools.partial(weighted_rows, ext, wts, acc, 2, deg))
    z_out[...] = join_parts(acc, z_out.shape[0], 2)


def index_scratch(deg):
    return [pltpu.SemaphoreType.DMA((CHUNKS,))] + [pltpu.SMEM((CHUNK_ROWS * deg,), I32)] * CHUNKS


def layer_one(src, wts, own, halo, deg):
    rows, halo_rows = own.shape[0], halo.shape[0] * halo.shape[1]
    step_rows = CHUNK_ROWS * CHUNKS
    return pl.pallas_call(
        functools.partial(layer_one_kernel, deg),
        grid=(rows // step_rows,),
        in_specs=[
            pl.BlockSpec(memory_space=pl.ANY),
            pl.BlockSpec((step_rows * deg, LANES), lambda i: (i, 0)),
            pl.BlockSpec((rows, 2 * LANES), lambda i: (0, 0)),
            pl.BlockSpec(halo.shape, lambda i: (0, 0, 0)),
        ],
        out_specs=pl.BlockSpec((step_rows, 2 * LANES), lambda i: (i, 0)),
        out_shape=jax.ShapeDtypeStruct((rows, 2 * LANES), BF16),
        scratch_shapes=[
            pltpu.VMEM(((rows + halo_rows) * 2, LANES), F32),
            pltpu.VMEM((step_rows * 2, LANES), F32),
        ] + index_scratch(deg),
        compiler_params=params(),
        name="layer_one",
    )(src, wts, own, halo)


def hidden_rows(z, w):
    return jnp.maximum(jnp.dot(z, w, preferred_element_type=F32), 0.0).astype(BF16)


def spread_hidden(ext, load, count, w_ref, base):
    parts = w_ref.shape[1] // LANES
    block = HIDDEN_ROWS

    def body(i, _):
        r = pl.multiple_of(i * block, block)
        h = hidden_rows(load(r, block), w_ref[...]).astype(F32)
        for c in range(parts):
            ext[pl.ds((base + r) * parts + c, block, stride=parts), :] = h[:, c * LANES:(c + 1) * LANES]
        return 0

    lax.fori_loop(0, count // block, body, 0)


def layer_two_kernel(deg, classes, src, wts, own, halo, w1, w2, lab, cnt, g_out, gw_out, loss_out, ext, acc, sems, *bufs):
    parts = w1.shape[1] // LANES
    step = pl.program_id(0)

    @pl.when(step == 0)
    def _():
        count = own.shape[0]
        spread_hidden(ext, lambda r, n: own[pl.ds(r, n), :], count, w1, 0)
        spread_lists(acc, halo, 0, 2)
        pair = lambda r, n: [acc[pl.ds(2 * r + c, n, stride=2), :].astype(BF16) for c in range(2)]
        spread_hidden(ext, lambda r, n: jnp.concatenate(pair(r, n), axis=1), halo.shape[0] * halo.shape[1], w1, count)
        gw_out[...] = jnp.zeros_like(gw_out)
        loss_out[...] = jnp.zeros_like(loss_out)

    with_indices(src, bufs, sems, functools.partial(weighted_rows, ext, wts, acc, parts, deg))

    rows = g_out.shape[0]
    z = join_parts(acc, rows, parts)
    logits = jnp.dot(z, w2[...], preferred_element_type=F32)
    col = lax.broadcasted_iota(I32, logits.shape, 1)
    real = col < classes
    peak = jnp.max(jnp.where(real, logits, -jnp.inf), axis=1, keepdims=True)
    shifted = logits - peak
    norm = jnp.log(jnp.sum(jnp.where(real, jnp.exp(shifted), 0.0), axis=1, keepdims=True))
    log_prob = shifted - norm
    label = lab[...]
    hit = col == label
    mask = (label >= 0).astype(F32)
    loss_out[...] += jnp.sum(jnp.where(hit, log_prob, 0.0).reshape(rows // 8, 8, LANES), axis=0)
    prob = jnp.where(real, jnp.exp(log_prob), 0.0)
    grad = ((prob - hit.astype(F32)) * (mask / cnt[0:1, :])).astype(BF16)
    g_out[...] = grad.astype(F32)
    gw_out[...] += lax.dot_general(z, grad, (((0,), (0,)), ((), ())), preferred_element_type=F32)


def layer_two(src, wts, own, halo, w1, w2, lab, cnt, deg, classes):
    rows, halo_rows, hid = own.shape[0], halo.shape[0] * halo.shape[1], w1.shape[1]
    step_rows = CHUNK_ROWS * CHUNKS
    parts = hid // LANES
    whole = lambda a: pl.BlockSpec(a.shape, lambda i: (0, 0))
    return pl.pallas_call(
        functools.partial(layer_two_kernel, deg, classes),
        grid=(rows // step_rows,),
        in_specs=[
            pl.BlockSpec(memory_space=pl.ANY),
            pl.BlockSpec((step_rows * deg, LANES), lambda i: (i, 0)),
            whole(own), pl.BlockSpec(halo.shape, lambda i: (0, 0, 0)), whole(w1), whole(w2),
            pl.BlockSpec((step_rows, 1), lambda i: (i, 0)),
            whole(cnt),
        ],
        out_specs=[
            pl.BlockSpec((step_rows, LANES), lambda i: (i, 0)),
            pl.BlockSpec((hid, LANES), lambda i: (0, 0)),
            pl.BlockSpec((8, LANES), lambda i: (0, 0)),
        ],
        out_shape=[
            jax.ShapeDtypeStruct((rows, LANES), F32),
            jax.ShapeDtypeStruct((hid, LANES), F32),
            jax.ShapeDtypeStruct((8, LANES), F32),
        ],
        scratch_shapes=[
            pltpu.VMEM(((rows + halo_rows) * parts, LANES), F32),
            pltpu.VMEM((step_rows * parts, LANES), F32),
        ] + index_scratch(deg),
        compiler_params=params(),
        name="layer_two",
    )(src, wts, own, halo, w1, w2, lab, cnt)


def fill_zero(refs, rows):
    def body(i, _):
        for ref in refs:
            ref[pl.ds(pl.multiple_of(i * 64, 64), 64), :] = jnp.zeros((64, LANES), F32)
        return 0

    lax.fori_loop(0, rows // 64, body, 0)


def tree_sum(vals):
    while len(vals) > 1:
        vals = [vals[i] + vals[i + 1] for i in range(0, len(vals) - 1, 2)] + ([vals[-1]] if len(vals) % 2 else [])
    return vals[0]


def scatter_kernel(deg, src, wts, grad, out, halo_out, sems, *rest):
    bufs, accs = rest[:CHUNKS], rest[CHUNKS:]
    step = pl.program_id(0)

    @pl.when(step == 0)
    def _():
        fill_zero(accs, accs[0].shape[0])

    def visit(b, idx):
        for n in range(CHUNK_ROWS):
            row = grad[pl.ds(b * CHUNK_ROWS + n, 1), :]
            todo = []
            for k in range(deg):
                at = idx[n * deg + k]
                term = row * wts[pl.ds((b * CHUNK_ROWS + n) * deg + k, 1), :]
                todo.append((accs[k], at, accs[k][pl.ds(at, 1), :] + term))
            for ref, at, val in todo:
                ref[pl.ds(at, 1), :] = val

    with_indices(src, bufs, sems, visit)

    @pl.when(step == pl.num_programs(0) - 1)
    def _():
        def body(i, _):
            s = pl.ds(pl.multiple_of(i * 64, 64), 64)
            out[s, :] = tree_sum([a[s, :] for a in accs])
            return 0

        rows = out.shape[0]
        lax.fori_loop(0, rows // 64, body, 0)
        count, size = halo_out.shape[:2]

        def lists(i, _):
            for u in range(16):
                s = pl.ds(pl.multiple_of(rows + (i * 16 + u) * size, size), size)
                halo_out[i * 16 + u] = tree_sum([a[s, :] for a in accs])
            return 0

        lax.fori_loop(0, count // 16, lists, 0)


def scatter_back(src, wts, grad, count, size, deg):
    rows = grad.shape[0]
    ext_rows = rows + count * size
    step_rows = CHUNK_ROWS * CHUNKS
    return pl.pallas_call(
        functools.partial(scatter_kernel, deg),
        grid=(rows // step_rows,),
        in_specs=[
            pl.BlockSpec(memory_space=pl.ANY),
            pl.BlockSpec((step_rows * deg, LANES), lambda i: (i, 0)),
            pl.BlockSpec((step_rows, LANES), lambda i: (i, 0)),
        ],
        out_specs=[
            pl.BlockSpec((rows, LANES), lambda i: (0, 0)),
            pl.BlockSpec((count, size, LANES), lambda i: (0, 0, 0)),
        ],
        out_shape=[
            jax.ShapeDtypeStruct((rows, LANES), F32),
            jax.ShapeDtypeStruct((count, size, LANES), F32),
        ],
        scratch_shapes=index_scratch(deg) + [pltpu.VMEM((ext_rows, LANES), F32)] * deg,
        compiler_params=params(),
        name="scatter_back",
    )(src, wts, grad)


def first_grad_kernel(lists, idx, agg, back, z_ref, w1, w2t, out, *accs):
    rows = agg.shape[0]
    spare = accs[0].shape[0] - rows
    fill_zero(accs, rows)
    for a in accs:
        a[pl.ds(rows, spare), :] = jnp.zeros((spare, LANES), F32)

    def fold(i, _):
        lo = idx.at[pl.ds(pl.multiple_of(i * 128, 128), 128)]
        for u in range(0, 128, lists):
            got = back.at[i * (128 // lists) + u // lists]
            todo = [(accs[j], lo[u + j], accs[j][pl.ds(lo[u + j], 1), :] + got[pl.ds(j, 1), :]) for j in range(lists)]
            for ref, at, val in todo:
                ref[pl.ds(at, 1), :] = val
        return 0

    lax.fori_loop(0, idx.shape[0] // 128, fold, 0)
    out[...] = jnp.zeros_like(out)
    block = 512

    def body(i, _):
        s = pl.ds(pl.multiple_of(i * block, block), block)
        p = agg[s, :] + tree_sum([a[s, :] for a in accs])
        hi = p.astype(BF16)
        rest = p - hi.astype(F32)
        mid = rest.astype(BF16)
        low = (rest - mid.astype(F32)).astype(BF16)
        dh = jnp.dot(jnp.concatenate([low, mid, hi], axis=1), w2t[...], preferred_element_type=F32)
        z = z_ref[s, :]
        h = hidden_rows(z, w1[...]).astype(F32)
        g = jnp.where(h > 0, dh, 0.0).astype(BF16)
        out[...] += lax.dot_general(z, g, (((0,), (0,)), ((), ())), preferred_element_type=F32)
        return 0

    lax.fori_loop(0, rows // block, body, 0)


def first_grad(idx, agg, back, z, w1, w2t, lists):
    rows = z.shape[0]
    vm = pl.BlockSpec(memory_space=pltpu.VMEM)
    return pl.pallas_call(
        functools.partial(first_grad_kernel, lists),
        grid=(1,),
        in_specs=[
            pl.BlockSpec(memory_space=pltpu.SMEM),
            pl.BlockSpec((rows, LANES), lambda i: (0, 0)),
            vm, vm, vm, vm,
        ],
        out_specs=vm,
        out_shape=jax.ShapeDtypeStruct((z.shape[1], w1.shape[1]), F32),
        scratch_shapes=[pltpu.VMEM((rows + 8, LANES), F32)] * lists,
        compiler_params=params(),
        name="first_grad",
    )(idx, agg, back, z, w1, w2t)


def place():
    me = lax.axis_index("graph")
    return lax.rem(me, 2), lax.rem(me // 2, 4), lax.rem(me // 8, 4), me // 32


def index_of(c, x, y, z):
    return ((z * 4 + y) * 4 + x) * 2 + c


def ring_peers(zs):
    c, x, y, z = place()
    return (
        [index_of(1 - c, x, y, z)],
        [index_of(c, lax.rem(x + d, 4), y, z) for d in range(1, 4)],
        [index_of(c, x, lax.rem(y + d, 4), z) for d in range(1, 4)],
        [index_of(c, x, y, lax.rem(z + d, zs)) for d in range(1, zs)],
    )


def greet(groups):
    barrier = pltpu.get_barrier_semaphore()
    peers = [p for g in groups for p in g]
    for p in peers:
        pl.semaphore_signal(barrier, inc=1, device_id=(p,), device_id_type=MESH)
    pl.semaphore_wait(barrier, len(peers))


def count_kernel(zs, val, out, mine, got, send, recv):
    groups = ring_peers(zs)
    greet(groups)
    mine[0] = val[...]
    slot = 0
    for s, peers in enumerate(groups):
        copies = []
        for p in peers:
            copies.append(pltpu.make_async_remote_copy(
                src_ref=mine.at[s], dst_ref=got.at[slot], send_sem=send.at[slot], recv_sem=recv.at[slot],
                device_id=(p,), device_id_type=MESH))
            slot += 1
        for copy in copies:
            copy.start()
        for copy in copies:
            copy.wait()
        mine[s + 1] = mine[s] + tree_sum([got[slot - len(peers) + i] for i in range(len(peers))])
    out[...] = mine[len(groups)]


def count_all(val, zs):
    n = 1 + 3 + 3 + zs - 1
    return pl.pallas_call(
        functools.partial(count_kernel, zs),
        in_specs=[pl.BlockSpec(memory_space=pltpu.VMEM)],
        out_specs=pl.BlockSpec(memory_space=pltpu.VMEM),
        out_shape=jax.ShapeDtypeStruct(val.shape, F32),
        scratch_shapes=[
            pltpu.VMEM((5,) + val.shape, F32), pltpu.VMEM((n,) + val.shape, F32),
            pltpu.SemaphoreType.DMA((n,)), pltpu.SemaphoreType.DMA((n,)),
        ],
        compiler_params=pltpu.CompilerParams(collective_id=1, has_side_effects=True),
        name="count_all",
    )(val)


def sum_kernel(zs, parts, g1, g2, loss, cnt, o_g1, o_g2, o_loss, val, s1, s2, s3, r1, r2, r3, r4, o0, o1, o2, send, recv):
    c, x, y, z = place()
    cores, xs, ys, zps = groups = ring_peers(zs)
    feat, hid = o_g1.shape[0], g2.shape[0]
    first = parts * feat
    for p in range(parts):
        val[pl.ds(p * feat, feat), :] = g1[pl.ds(0, feat), p * LANES:(p + 1) * LANES]
    val[pl.ds(first, hid), :] = g2[...]
    val[pl.ds(first + hid, 8), :] = loss[...]
    spare = val.shape[0] - first - hid - 8
    val[pl.ds(first + hid + 8, spare), :] = jnp.zeros((spare, LANES), F32)
    greet(groups)
    h, q, e = r1.shape[0], s2.shape[1], s3.shape[1]
    used = [0]

    def remote(src, dst, peer):
        i = used[0]
        used[0] += 1
        return pltpu.make_async_remote_copy(
            src_ref=src, dst_ref=dst, send_sem=send.at[i], recv_sem=recv.at[i], device_id=(peer,), device_id_type=MESH)

    def run(copies):
        for copy in copies:
            copy.start()
        for copy in copies:
            copy.wait()

    def at(i, size, base=0):
        return pl.ds(pl.multiple_of(base + i * size, 8), size)

    routes = ((x, xs, y, ys), (y, ys, x, xs))
    half = h // 2
    run([remote(val.at[at(1 - c, h)], r1, cores[0])])
    s1[...] = val[at(c, h), :] + r1[...]
    run([remote(s1.at[at(lax.rem(a + d, 4), q, k * half)], r2.at[k, d - 1], pa[d - 1])
         for d in range(1, 4) for k, (a, pa, _, _) in enumerate(routes)])
    for k, (a, _, _, _) in enumerate(routes):
        s2[k] = (s1[at(a, q, k * half), :] + r2[k, 0]) + (r2[k, 1] + r2[k, 2])
    run([remote(s2.at[k, at(lax.rem(b + d, 4), e)], r3.at[k, d - 1], pb[d - 1])
         for d in range(1, 4) for k, (_, _, b, pb) in enumerate(routes)])
    for k, (_, _, b, _) in enumerate(routes):
        s3[k] = (s2[k, at(b, e), :] + r3[k, 0]) + (r3[k, 1] + r3[k, 2])
    r4[z] = s3[...]
    run([remote(s3, r4.at[z], zps[d - 1]) for d in range(1, zs)])
    for k, (_, _, b, _) in enumerate(routes):
        o2[k, at(b, e), :] = tree_sum([r4[i, k] for i in range(zs)])
    run([remote(o2.at[k, at(b, e)], o2.at[k, at(b, e)], pb[d - 1])
         for d in range(1, 4) for k, (_, _, b, pb) in enumerate(routes)])
    for k, (a, _, _, _) in enumerate(routes):
        o1[at(a, q, k * half), :] = o2[k]
    run([remote(o2.at[k], o1.at[at(a, q, k * half)], pa[d - 1])
         for d in range(1, 4) for k, (a, pa, _, _) in enumerate(routes)])
    o0[at(c, h), :] = o1[...]
    run([remote(o1, o0.at[at(c, h)], cores[0])])
    for p in range(parts):
        o_g1[:, p * LANES:(p + 1) * LANES] = o0[pl.ds(p * feat, feat), :]
    o_g2[...] = o0[pl.ds(first, hid), :]
    total = jnp.sum(o0[pl.ds(first + hid, 8), :], axis=0, keepdims=True)
    o_loss[...] = jnp.broadcast_to(-jnp.sum(total, axis=1, keepdims=True) / cnt[0:1, :], o_loss.shape)


def sum_all(g1, g2, loss, cnt, feat, zs):
    hid = g1.shape[1]
    parts = hid // LANES
    used = parts * feat + g2.shape[0] + 8
    rows = used + -used % 512
    h, q, e = rows // 2, rows // 16, rows // 64
    n = 2 * (1 + 6 + 6) + zs - 1
    buf = lambda *s: pltpu.VMEM(s + (LANES,), F32)
    vm = pl.BlockSpec(memory_space=pltpu.VMEM)
    return pl.pallas_call(
        functools.partial(sum_kernel, zs, parts),
        in_specs=[vm] * 4,
        out_specs=[vm] * 3,
        out_shape=[
            jax.ShapeDtypeStruct((feat, hid), F32),
            jax.ShapeDtypeStruct(g2.shape, F32),
            jax.ShapeDtypeStruct((8, LANES), F32),
        ],
        scratch_shapes=[
            buf(rows), buf(h), buf(2, q), buf(2, e), buf(h), buf(2, 3, q), buf(2, 3, e), buf(zs, 2, e),
            buf(rows), buf(h), buf(2, q),
            pltpu.SemaphoreType.DMA((n,)), pltpu.SemaphoreType.DMA((n,)),
        ],
        compiler_params=pltpu.CompilerParams(collective_id=0, has_side_effects=True, vmem_limit_bytes=32 * 2**20),
        name="sum_all",
    )(g1, g2, loss, cnt)


def solution(mesh):
    devs = mesh.shape["graph"]
    zs = devs // 32

    def device_step(feats, w_one, w_two, send_idx, send_count, edge_src, edge_wt, labels, label_mask):
        rows, feat_in = feats.shape
        hid, classes = w_two.shape
        lists, deg = send_idx.shape[1], edge_src.shape[1]

        list_ok = jnp.arange(lists)[None, :] < send_count[:, None]
        list_rows = jnp.where(list_ok, send_idx, rows).reshape(devs * lists)
        src = edge_src.reshape(rows * deg)
        wts = jnp.broadcast_to(edge_wt[:, :, None], (rows, deg, LANES)).reshape(rows * deg, LANES)
        w1 = jnp.pad(w_one.astype(BF16), ((0, 2 * LANES - feat_in), (0, 0)))
        w2 = jnp.pad(w_two.astype(BF16), ((0, 0), (0, LANES - classes)))
        own = jnp.pad(feats, ((0, 0), (0, 2 * LANES - feat_in)))
        lab = jnp.where(label_mask == 1, labels, -1)[:, None]
        local_count = jnp.broadcast_to(jnp.sum(label_mask.astype(F32)), (8, LANES))

        def exchange(block):
            return lax.all_to_all(block, "graph", 0, 0, tiled=True)

        halo_one = exchange(pick_rows(list_rows * 2, own, lists))
        cnt = count_all(local_count, zs)
        z_one = layer_one(src * 2, wts, own, halo_one, deg)
        halo_two = exchange(pick_rows(list_rows * 2, z_one, lists))
        grad, gw_two, loss_part = layer_two(src * (hid // LANES), wts, z_one, halo_two, w1, w2, lab, cnt, deg, classes)
        agg, halo_grad = scatter_back(src, wts, grad, devs, lists, deg)
        back = exchange(halo_grad)
        gw_one = first_grad(list_rows, agg, back, z_one, w1, jnp.tile(w2.T, (3, 1)), lists)

        grad_one, grad_two, loss = sum_all(gw_one, gw_two, loss_part, cnt, feat_in, zs)
        return loss[0, 0], grad_one, grad_two[:, :classes]

    row_spec = P("graph", None)
    vec_spec = P("graph")

    return jax.shard_map(device_step, mesh=mesh, in_specs=(row_spec, P(), P(), row_spec, vec_spec, row_spec, row_spec, vec_spec, vec_spec), out_specs=(P(), P(), P()), check_vma=False)
```

```python
import functools

import jax
import jax.numpy as jnp
from jax import lax
from jax.experimental import pallas as pl
from jax.experimental.pallas import tpu as pltpu
from jax.sharding import PartitionSpec as P


F32, BF16, I32 = jnp.float32, jnp.bfloat16, jnp.int32
LANES = 128
CHUNK_ROWS = 128
HIDDEN_ROWS = 512
CHUNKS = 4
VMEM_CAP = 60 * 2**20
MESH = pl.DeviceIdType.MESH


def params(**kw):
    return pltpu.CompilerParams(vmem_limit_bytes=VMEM_CAP, **kw)


def spread_rows(dst, rows_ref, base, width):
    parts = width // LANES
    count = rows_ref.shape[0]

    block = 128

    def body(i, _):
        r = pl.multiple_of(i * block, block)
        vals = rows_ref[pl.ds(r, block), :].astype(F32)
        for c in range(parts):
            dst[pl.ds((base + r) * parts + c, block, stride=parts), :] = vals[:, c * LANES:(c + 1) * LANES]
        return 0

    lax.fori_loop(0, count // block, body, 0)


def spread_lists(dst, lists_ref, base, parts):
    count, size = lists_ref.shape[:2]
    group = 16

    def body(i, _):
        for u in range(group):
            q = i * group + u
            vals = lists_ref[q].astype(F32)
            for c in range(parts):
                dst[pl.ds((base + q * size) * parts + c, size, stride=parts), :] = vals[:, c * LANES:(c + 1) * LANES]
        return 0

    lax.fori_loop(0, count // group, body, 0)


def join_parts(src, rows, parts):
    return jnp.concatenate([src[pl.ds(c, rows, stride=parts), :].astype(BF16) for c in range(parts)], axis=1)


def pick_kernel(idx, rows_ref, out, ext, stage):
    count = rows_ref.shape[0]
    lists, size = out.shape[:2]
    picks = lists * size
    gap = picks + 8
    group = 128 // size
    ext[pl.ds(2 * count, 8), :] = jnp.zeros((8, LANES), F32)
    spread_rows(ext, rows_ref, 0, 2 * LANES)

    def body(i, _):
        lo = idx.at[pl.ds(pl.multiple_of(i * 128, 128), 128)]
        for u in range(128):
            stage[pl.ds(i * 128 + u, 2, stride=gap), :] = ext[pl.ds(pl.multiple_of(lo[u], 2), 2), :]
        for u in range(group):
            for c in range(2):
                vals = stage[pl.ds(c * gap + i * 128 + u * size, size), :]
                out[i * group + u, :, c * LANES:(c + 1) * LANES] = vals.astype(BF16)
        return 0

    lax.fori_loop(0, picks // 128, body, 0)


def pick_rows(idx, rows, size):
    picks, count = idx.shape[0], rows.shape[0]
    return pl.pallas_call(
        pick_kernel,
        in_specs=[pl.BlockSpec(memory_space=pltpu.SMEM), pl.BlockSpec(memory_space=pltpu.VMEM)],
        out_specs=pl.BlockSpec(memory_space=pltpu.VMEM),
        out_shape=jax.ShapeDtypeStruct((picks // size, size, 2 * LANES), BF16),
        scratch_shapes=[pltpu.VMEM((2 * count + 8, LANES), F32), pltpu.VMEM((2 * (picks + 8), LANES), F32)],
        compiler_params=params(),
        name="pick_rows",
    )(idx, rows)


def index_copies(step, src, bufs, sems):
    size = bufs[0].shape[0]
    return [
        pltpu.make_async_copy(src.at[pl.ds(pl.multiple_of((step * CHUNKS + b) * size, size), size)], bufs[b], sems.at[b])
        for b in range(CHUNKS)
    ]


def with_indices(src, bufs, sems, visit):
    step, last = pl.program_id(0), pl.num_programs(0) - 1
    now, later = index_copies(step, src, bufs, sems), index_copies(step + 1, src, bufs, sems)

    @pl.when(step == 0)
    def _():
        for copy in now:
            copy.start()

    for b in range(CHUNKS):
        now[b].wait()
        visit(b, bufs[b])

        @pl.when(step < last)
        def _():
            later[b].start()


def weighted_rows(ext, wts, acc, parts, deg, b, idx):
    for n in range(CHUNK_ROWS):
        total = None
        for k in range(deg):
            row = ext[pl.ds(pl.multiple_of(idx[n * deg + k], parts), parts), :]
            term = row * wts[pl.ds((b * CHUNK_ROWS + n) * deg + k, 1), :]
            total = term if total is None else total + term
        acc[pl.ds((b * CHUNK_ROWS + n) * parts, parts), :] = total


def spread_kernel(wt, out):
    deg = wt.shape[0]
    for n in range(wt.shape[1]):
        out[pl.ds(n * deg, deg), :] = jnp.broadcast_to(wt[:, n:n + 1], (deg, LANES))


def spread_weights(wt):
    deg, rows = wt.shape
    block = 512
    return pl.pallas_call(
        spread_kernel,
        grid=(rows // block,),
        in_specs=[pl.BlockSpec((deg, block), lambda i: (0, i))],
        out_specs=pl.BlockSpec((block * deg, LANES), lambda i: (i, 0)),
        out_shape=jax.ShapeDtypeStruct((rows * deg, LANES), F32),
        cost_estimate=pl.CostEstimate(flops=0, bytes_accessed=rows * deg * LANES * 4, transcendentals=0),
        compiler_params=params(),
        name="spread_weights",
    )(wt)


def layer_one_kernel(deg, src, wts, own, halo, z_out, ext, acc, sems, *bufs):
    @pl.when(pl.program_id(0) == 0)
    def _():
        spread_rows(ext, own, 0, 2 * LANES)
        spread_lists(ext, halo, own.shape[0], 2)

    with_indices(src, bufs, sems, functools.partial(weighted_rows, ext, wts, acc, 2, deg))
    z_out[...] = join_parts(acc, z_out.shape[0], 2)


def index_scratch(deg):
    return [pltpu.SemaphoreType.DMA((CHUNKS,))] + [pltpu.SMEM((CHUNK_ROWS * deg,), I32)] * CHUNKS


def layer_one(src, wts, own, halo, deg):
    rows, halo_rows = own.shape[0], halo.shape[0] * halo.shape[1]
    step_rows = CHUNK_ROWS * CHUNKS
    return pl.pallas_call(
        functools.partial(layer_one_kernel, deg),
        grid=(rows // step_rows,),
        in_specs=[
            pl.BlockSpec(memory_space=pl.ANY),
            pl.BlockSpec((step_rows * deg, LANES), lambda i: (i, 0)),
            pl.BlockSpec((rows, 2 * LANES), lambda i: (0, 0)),
            pl.BlockSpec(halo.shape, lambda i: (0, 0, 0)),
        ],
        out_specs=pl.BlockSpec((step_rows, 2 * LANES), lambda i: (i, 0)),
        out_shape=jax.ShapeDtypeStruct((rows, 2 * LANES), BF16),
        scratch_shapes=[
            pltpu.VMEM(((rows + halo_rows) * 2, LANES), F32),
            pltpu.VMEM((step_rows * 2, LANES), F32),
        ] + index_scratch(deg),
        compiler_params=params(),
        name="layer_one",
    )(src, wts, own, halo)


def hidden_rows(z, w):
    return jnp.maximum(jnp.dot(z, w, preferred_element_type=F32), 0.0).astype(BF16)


def spread_hidden(ext, load, count, w_ref, base):
    parts = w_ref.shape[1] // LANES
    block = HIDDEN_ROWS

    def body(i, _):
        r = pl.multiple_of(i * block, block)
        h = hidden_rows(load(r, block), w_ref[...]).astype(F32)
        for c in range(parts):
            ext[pl.ds((base + r) * parts + c, block, stride=parts), :] = h[:, c * LANES:(c + 1) * LANES]
        return 0

    lax.fori_loop(0, count // block, body, 0)


def layer_two_kernel(deg, classes, src, wts, own, halo, w1, w2, lab, cnt, g_out, gw_out, loss_out, ext, acc, sems, *bufs):
    parts = w1.shape[1] // LANES
    step = pl.program_id(0)

    @pl.when(step == 0)
    def _():
        count = own.shape[0]
        spread_hidden(ext, lambda r, n: own[pl.ds(r, n), :], count, w1, 0)
        spread_lists(acc, halo, 0, 2)
        pair = lambda r, n: [acc[pl.ds(2 * r + c, n, stride=2), :].astype(BF16) for c in range(2)]
        spread_hidden(ext, lambda r, n: jnp.concatenate(pair(r, n), axis=1), halo.shape[0] * halo.shape[1], w1, count)
        gw_out[...] = jnp.zeros_like(gw_out)
        loss_out[...] = jnp.zeros_like(loss_out)

    with_indices(src, bufs, sems, functools.partial(weighted_rows, ext, wts, acc, parts, deg))

    rows = g_out.shape[0]
    z = join_parts(acc, rows, parts)
    logits = jnp.dot(z, w2[...], preferred_element_type=F32)
    col = lax.broadcasted_iota(I32, logits.shape, 1)
    real = col < classes
    peak = jnp.max(jnp.where(real, logits, -jnp.inf), axis=1, keepdims=True)
    shifted = logits - peak
    norm = jnp.log(jnp.sum(jnp.where(real, jnp.exp(shifted), 0.0), axis=1, keepdims=True))
    log_prob = shifted - norm
    label = lab[...]
    hit = col == label
    mask = (label >= 0).astype(F32)
    loss_out[...] += jnp.sum(jnp.where(hit, log_prob, 0.0).reshape(rows // 8, 8, LANES), axis=0)
    prob = jnp.where(real, jnp.exp(log_prob), 0.0)
    grad = ((prob - hit.astype(F32)) * (mask / cnt[0:1, :])).astype(BF16)
    g_out[...] = grad.astype(F32)
    gw_out[...] += lax.dot_general(grad, z, (((0,), (0,)), ((), ())), preferred_element_type=F32)


def layer_two(src, wts, own, halo, w1, w2, lab, cnt, deg, classes):
    rows, halo_rows, hid = own.shape[0], halo.shape[0] * halo.shape[1], w1.shape[1]
    step_rows = CHUNK_ROWS * CHUNKS
    parts = hid // LANES
    whole = lambda a: pl.BlockSpec(a.shape, lambda i: (0, 0))
    return pl.pallas_call(
        functools.partial(layer_two_kernel, deg, classes),
        grid=(rows // step_rows,),
        in_specs=[
            pl.BlockSpec(memory_space=pl.ANY),
            pl.BlockSpec((step_rows * deg, LANES), lambda i: (i, 0)),
            whole(own), pl.BlockSpec(halo.shape, lambda i: (0, 0, 0)), whole(w1), whole(w2),
            pl.BlockSpec((step_rows, 1), lambda i: (i, 0)),
            whole(cnt),
        ],
        out_specs=[
            pl.BlockSpec((step_rows, LANES), lambda i: (i, 0)),
            pl.BlockSpec((LANES, hid), lambda i: (0, 0)),
            pl.BlockSpec((8, LANES), lambda i: (0, 0)),
        ],
        out_shape=[
            jax.ShapeDtypeStruct((rows, LANES), F32),
            jax.ShapeDtypeStruct((LANES, hid), F32),
            jax.ShapeDtypeStruct((8, LANES), F32),
        ],
        scratch_shapes=[
            pltpu.VMEM(((rows + halo_rows) * parts, LANES), F32),
            pltpu.VMEM((step_rows * parts, LANES), F32),
        ] + index_scratch(deg),
        compiler_params=params(),
        name="layer_two",
    )(src, wts, own, halo, w1, w2, lab, cnt)


def fill_zero(refs, rows):
    def body(i, _):
        for ref in refs:
            ref[pl.ds(pl.multiple_of(i * 64, 64), 64), :] = jnp.zeros((64, LANES), F32)
        return 0

    lax.fori_loop(0, rows // 64, body, 0)


def tree_sum(vals):
    while len(vals) > 1:
        vals = [vals[i] + vals[i + 1] for i in range(0, len(vals) - 1, 2)] + ([vals[-1]] if len(vals) % 2 else [])
    return vals[0]


def scatter_kernel(deg, src, wts, grad, out, halo_out, sems, *rest):
    bufs, accs = rest[:CHUNKS], rest[CHUNKS:]
    step = pl.program_id(0)

    @pl.when(step == 0)
    def _():
        fill_zero(accs, accs[0].shape[0])

    def visit(b, idx):
        for n in range(CHUNK_ROWS):
            row = grad[pl.ds(b * CHUNK_ROWS + n, 1), :]
            todo = []
            for k in range(deg):
                at = idx[n * deg + k]
                term = row * wts[pl.ds((b * CHUNK_ROWS + n) * deg + k, 1), :]
                todo.append((accs[k], at, accs[k][pl.ds(at, 1), :] + term))
            for ref, at, val in todo:
                ref[pl.ds(at, 1), :] = val

    with_indices(src, bufs, sems, visit)

    @pl.when(step == pl.num_programs(0) - 1)
    def _():
        def body(i, _):
            s = pl.ds(pl.multiple_of(i * 64, 64), 64)
            out[s, :] = tree_sum([a[s, :] for a in accs])
            return 0

        rows = out.shape[0]
        lax.fori_loop(0, rows // 64, body, 0)
        count, size = halo_out.shape[:2]

        def lists(i, _):
            for u in range(16):
                s = pl.ds(pl.multiple_of(rows + (i * 16 + u) * size, size), size)
                halo_out[i * 16 + u] = tree_sum([a[s, :] for a in accs])
            return 0

        lax.fori_loop(0, count // 16, lists, 0)


def scatter_back(src, wts, grad, count, size, deg):
    rows = grad.shape[0]
    ext_rows = rows + count * size
    step_rows = CHUNK_ROWS * CHUNKS
    return pl.pallas_call(
        functools.partial(scatter_kernel, deg),
        grid=(rows // step_rows,),
        in_specs=[
            pl.BlockSpec(memory_space=pl.ANY),
            pl.BlockSpec((step_rows * deg, LANES), lambda i: (i, 0)),
            pl.BlockSpec((step_rows, LANES), lambda i: (i, 0)),
        ],
        out_specs=[
            pl.BlockSpec((rows, LANES), lambda i: (0, 0)),
            pl.BlockSpec((count, size, LANES), lambda i: (0, 0, 0)),
        ],
        out_shape=[
            jax.ShapeDtypeStruct((rows, LANES), F32),
            jax.ShapeDtypeStruct((count, size, LANES), F32),
        ],
        scratch_shapes=index_scratch(deg) + [pltpu.VMEM((ext_rows, LANES), F32)] * deg,
        compiler_params=params(),
        name="scatter_back",
    )(src, wts, grad)


def first_grad_kernel(lists, idx, agg, back, z_ref, w1, w2t, out, *accs):
    rows = agg.shape[0]
    spare = accs[0].shape[0] - rows
    fill_zero(accs, rows)
    for a in accs:
        a[pl.ds(rows, spare), :] = jnp.zeros((spare, LANES), F32)

    def fold(i, _):
        lo = idx.at[pl.ds(pl.multiple_of(i * 128, 128), 128)]
        for u in range(0, 128, lists):
            got = back.at[i * (128 // lists) + u // lists]
            todo = [(accs[j], lo[u + j], accs[j][pl.ds(lo[u + j], 1), :] + got[pl.ds(j, 1), :]) for j in range(lists)]
            for ref, at, val in todo:
                ref[pl.ds(at, 1), :] = val
        return 0

    lax.fori_loop(0, idx.shape[0] // 128, fold, 0)
    out[...] = jnp.zeros_like(out)
    block = 512

    def body(i, _):
        s = pl.ds(pl.multiple_of(i * block, block), block)
        p = agg[s, :] + tree_sum([a[s, :] for a in accs])
        hi = p.astype(BF16)
        rest = p - hi.astype(F32)
        mid = rest.astype(BF16)
        low = (rest - mid.astype(F32)).astype(BF16)
        dh = jnp.dot(jnp.concatenate([low, mid, hi], axis=1), w2t[...], preferred_element_type=F32)
        z = z_ref[s, :]
        h = hidden_rows(z, w1[...]).astype(F32)
        g = jnp.where(h > 0, dh, 0.0).astype(BF16)
        out[...] += lax.dot_general(z, g, (((0,), (0,)), ((), ())), preferred_element_type=F32)
        return 0

    lax.fori_loop(0, rows // block, body, 0)


def first_grad(idx, agg, back, z, w1, w2t, lists):
    rows = z.shape[0]
    vm = pl.BlockSpec(memory_space=pltpu.VMEM)
    return pl.pallas_call(
        functools.partial(first_grad_kernel, lists),
        grid=(1,),
        in_specs=[
            pl.BlockSpec(memory_space=pltpu.SMEM),
            pl.BlockSpec((rows, LANES), lambda i: (0, 0)),
            vm, vm, vm, vm,
        ],
        out_specs=vm,
        out_shape=jax.ShapeDtypeStruct((z.shape[1], w1.shape[1]), F32),
        scratch_shapes=[pltpu.VMEM((rows + 8, LANES), F32)] * lists,
        compiler_params=params(),
        name="first_grad",
    )(idx, agg, back, z, w1, w2t)


def place():
    me = lax.axis_index("graph")
    return lax.rem(me, 2), lax.rem(me // 2, 4), lax.rem(me // 8, 4), me // 32


def index_of(c, x, y, z):
    return ((z * 4 + y) * 4 + x) * 2 + c


def ring_peers(zs):
    c, x, y, z = place()
    return (
        [index_of(1 - c, x, y, z)],
        [index_of(c, lax.rem(x + d, 4), y, z) for d in range(1, 4)],
        [index_of(c, x, lax.rem(y + d, 4), z) for d in range(1, 4)],
        [index_of(c, x, y, lax.rem(z + d, zs)) for d in range(1, zs)],
    )


def greet(groups):
    barrier = pltpu.get_barrier_semaphore()
    peers = [p for g in groups for p in g]
    for p in peers:
        pl.semaphore_signal(barrier, inc=1, device_id=(p,), device_id_type=MESH)
    pl.semaphore_wait(barrier, len(peers))


def count_kernel(zs, val, out, mine, got, send, recv):
    c, x, y, z = place()
    plane = [index_of(lax.rem(c + i, 2), lax.rem(x + d, 4), y, z) for d in range(4) for i in range(2) if i or d]
    _, _, ys, zps = ring_peers(zs)
    groups = (plane, ys, zps)
    greet(groups)
    mine[0] = val[...]
    slot = 0
    for s, peers in enumerate(groups):
        copies = []
        for p in peers:
            copies.append(pltpu.make_async_remote_copy(
                src_ref=mine.at[s], dst_ref=got.at[slot], send_sem=send.at[slot], recv_sem=recv.at[slot],
                device_id=(p,), device_id_type=MESH))
            slot += 1
        for copy in copies:
            copy.start()
        for copy in copies:
            copy.wait()
        mine[s + 1] = mine[s] + tree_sum([got[slot - len(peers) + i] for i in range(len(peers))])
    out[...] = mine[len(groups)]


def count_all(val, zs):
    n = 7 + 3 + zs - 1
    return pl.pallas_call(
        functools.partial(count_kernel, zs),
        in_specs=[pl.BlockSpec(memory_space=pltpu.VMEM)],
        out_specs=pl.BlockSpec(memory_space=pltpu.VMEM),
        out_shape=jax.ShapeDtypeStruct(val.shape, F32),
        scratch_shapes=[
            pltpu.VMEM((4,) + val.shape, F32), pltpu.VMEM((n,) + val.shape, F32),
            pltpu.SemaphoreType.DMA((n,)), pltpu.SemaphoreType.DMA((n,)),
        ],
        compiler_params=pltpu.CompilerParams(collective_id=1, has_side_effects=True),
        name="count_all",
    )(val)


def sum_kernel(zs, parts, g1, g2, loss, cnt, o_g1, o_g2, o_loss, val, s1, s2, s3, r1, r2, r3, r4, o0, o1, o2, send, recv):
    c, x, y, z = place()
    cores, xs, ys, zps = groups = ring_peers(zs)
    feat, hid = o_g1.shape[0], parts * LANES
    first = parts * feat
    for p in range(parts):
        val[pl.ds(p * feat, feat), :] = g1[pl.ds(0, feat), p * LANES:(p + 1) * LANES]
    for p in range(parts):
        val[pl.ds(first + p * LANES, LANES), :] = g2[:, p * LANES:(p + 1) * LANES]
    val[pl.ds(first + hid, 8), :] = loss[...]
    spare = val.shape[0] - first - hid - 8
    val[pl.ds(first + hid + 8, spare), :] = jnp.zeros((spare, LANES), F32)
    greet(groups)
    h, q, e = r1.shape[0], s2.shape[1], s3.shape[1]
    used = [0]

    def remote(src, dst, peer):
        i = used[0]
        used[0] += 1
        return pltpu.make_async_remote_copy(
            src_ref=src, dst_ref=dst, send_sem=send.at[i], recv_sem=recv.at[i], device_id=(peer,), device_id_type=MESH)

    def run(copies):
        for copy in copies:
            copy.start()
        for copy in copies:
            copy.wait()

    def at(i, size, base=0):
        return pl.ds(pl.multiple_of(base + i * size, 8), size)

    routes = ((x, xs, y, ys), (y, ys, x, xs))
    half = h // 2
    run([remote(val.at[at(1 - c, h)], r1, cores[0])])
    s1[...] = val[at(c, h), :] + r1[...]
    run([remote(s1.at[at(lax.rem(a + d, 4), q, k * half)], r2.at[k, d - 1], pa[d - 1])
         for d in range(1, 4) for k, (a, pa, _, _) in enumerate(routes)])
    for k, (a, _, _, _) in enumerate(routes):
        s2[k] = (s1[at(a, q, k * half), :] + r2[k, 0]) + (r2[k, 1] + r2[k, 2])
    run([remote(s2.at[k, at(lax.rem(b + d, 4), e)], r3.at[k, d - 1], pb[d - 1])
         for d in range(1, 4) for k, (_, _, b, pb) in enumerate(routes)])
    for k, (_, _, b, _) in enumerate(routes):
        s3[k] = (s2[k, at(b, e), :] + r3[k, 0]) + (r3[k, 1] + r3[k, 2])
    r4[z] = s3[...]
    run([remote(s3, r4.at[z], zps[d - 1]) for d in range(1, zs)])
    for k, (_, _, b, _) in enumerate(routes):
        o2[k, at(b, e), :] = tree_sum([r4[i, k] for i in range(zs)])
    run([remote(o2.at[k, at(b, e)], o2.at[k, at(b, e)], pb[d - 1])
         for d in range(1, 4) for k, (_, _, b, pb) in enumerate(routes)])
    for k, (a, _, _, _) in enumerate(routes):
        o1[at(a, q, k * half), :] = o2[k]
    run([remote(o2.at[k], o1.at[at(a, q, k * half)], pa[d - 1])
         for d in range(1, 4) for k, (a, pa, _, _) in enumerate(routes)])
    o0[at(c, h), :] = o1[...]
    run([remote(o1, o0.at[at(c, h)], cores[0])])
    for p in range(parts):
        o_g1[:, p * LANES:(p + 1) * LANES] = o0[pl.ds(p * feat, feat), :]
    for p in range(parts):
        o_g2[:, p * LANES:(p + 1) * LANES] = o0[pl.ds(first + p * LANES, LANES), :]
    total = jnp.sum(o0[pl.ds(first + hid, 8), :], axis=0, keepdims=True)
    o_loss[...] = jnp.broadcast_to(-jnp.sum(total, axis=1, keepdims=True) / cnt[0:1, :], o_loss.shape)


def sum_all(g1, g2, loss, cnt, feat, zs):
    hid = g1.shape[1]
    parts = hid // LANES
    used = parts * feat + hid + 8
    rows = used + -used % 512
    h, q, e = rows // 2, rows // 16, rows // 64
    n = 2 * (1 + 6 + 6) + zs - 1
    buf = lambda *s: pltpu.VMEM(s + (LANES,), F32)
    vm = pl.BlockSpec(memory_space=pltpu.VMEM)
    return pl.pallas_call(
        functools.partial(sum_kernel, zs, parts),
        in_specs=[vm] * 4,
        out_specs=[vm] * 3,
        out_shape=[
            jax.ShapeDtypeStruct((feat, hid), F32),
            jax.ShapeDtypeStruct(g2.shape, F32),
            jax.ShapeDtypeStruct((8, LANES), F32),
        ],
        scratch_shapes=[
            buf(rows), buf(h), buf(2, q), buf(2, e), buf(h), buf(2, 3, q), buf(2, 3, e), buf(zs, 2, e),
            buf(rows), buf(h), buf(2, q),
            pltpu.SemaphoreType.DMA((n,)), pltpu.SemaphoreType.DMA((n,)),
        ],
        compiler_params=pltpu.CompilerParams(collective_id=0, has_side_effects=True, vmem_limit_bytes=32 * 2**20),
        name="sum_all",
    )(g1, g2, loss, cnt)


def solution(mesh):
    devs = mesh.shape["graph"]
    zs = devs // 32

    def device_step(feats, w_one, w_two, send_idx, send_count, edge_src, edge_wt, labels, label_mask):
        rows, feat_in = feats.shape
        hid, classes = w_two.shape
        lists, deg = send_idx.shape[1], edge_src.shape[1]

        list_ok = jnp.arange(lists)[None, :] < send_count[:, None]
        list_rows = jnp.where(list_ok, send_idx, rows).reshape(devs * lists)
        src = edge_src.reshape(rows * deg)
        wts = spread_weights(edge_wt.T)
        w1 = jnp.pad(w_one.astype(BF16), ((0, 2 * LANES - feat_in), (0, 0)))
        w2 = jnp.pad(w_two.astype(BF16), ((0, 0), (0, LANES - classes)))
        lab = jnp.where(label_mask == 1, labels, -1)[:, None]
        local_count = jnp.broadcast_to(jnp.sum(label_mask.astype(F32)), (8, LANES))
        own = jnp.pad(feats, ((0, 0), (0, 2 * LANES - feat_in)))

        def exchange(block):
            return lax.all_to_all(block, "graph", 0, 0, tiled=True)

        halo_one = exchange(pick_rows(list_rows * 2, own, lists))
        cnt = count_all(local_count, zs)
        z_one = layer_one(src * 2, wts, own, halo_one, deg)
        halo_two = exchange(pick_rows(list_rows * 2, z_one, lists))
        grad, gw_two, loss_part = layer_two(src * (hid // LANES), wts, z_one, halo_two, w1, w2, lab, cnt, deg, classes)
        agg, halo_grad = scatter_back(src, wts, grad, devs, lists, deg)
        w2t = jnp.tile(w2.T, (3, 1))
        back = exchange(halo_grad)
        gw_one = first_grad(list_rows, agg, back, z_one, w1, w2t, lists)

        grad_one, grad_two, loss = sum_all(gw_one, gw_two, loss_part, cnt, feat_in, zs)
        return loss[0, 0], grad_one, grad_two[:classes].T

    row_spec = P("graph", None)
    vec_spec = P("graph")

    return jax.shard_map(device_step, mesh=mesh, in_specs=(row_spec, P(), P(), row_spec, vec_spec, row_spec, row_spec, vec_spec, vec_spec), out_specs=(P(), P(), P()), check_vma=False)
```
